128 devices in a mesh: rep: 1, dp: 128 (over x, y, z, core).
Axes of the slice: x: 4, y: 4, z: 4, core: 2. Of those that a mesh axis runs over, the one named last changes fastest.
Arguments:
- x: bfloat16 [128, 1024, 1024], P(('rep', 'dp'))
- dy: bfloat16 [128, 1024, 1024], P(('rep', 'dp'))
- wq: bfloat16 [1, 1024, 1024], P(None, 'dp')
- wk: bfloat16 [1, 1024, 1024], P(None, 'dp')
- wv: bfloat16 [1, 1024, 1024], P(None, 'dp')
- wo: bfloat16 [1, 1024, 1024], P(None, 'dp')
- w_gate: bfloat16 [1, 1024, 3072], P(None, 'dp')
- w_up: bfloat16 [1, 1024, 3072], P(None, 'dp')
- w_down: bfloat16 [1, 3072, 1024], P(None, 'dp')
Outputs:
- output 1: bfloat16 [128, 1024, 1024], P(('rep', 'dp'))
- output 2: bfloat16 [1, 1024, 1024], P('rep', 'dp')
- output 3: bfloat16 [1, 1024, 1024], P('rep', 'dp')
- output 4: bfloat16 [1, 1024, 1024], P('rep', 'dp')
- output 5: bfloat16 [1, 1024, 1024], P('rep', 'dp')
- output 6: bfloat16 [1, 1024, 3072], P('rep', 'dp')
- output 7: bfloat16 [1, 1024, 3072], P('rep', 'dp')
- output 8: bfloat16 [1, 3072, 1024], P('rep', 'dp')
All inputs are finite; a program needn't handle non-finite values.
Results may differ from the reference program's by a relative error of at most 0.0295.
Values are sent between devices in bfloat16 or wider.
A program may use at most 1.5 GiB of HBM per device.

```python
import jax
import jax.numpy as jnp
from jax import lax

SEQUENCES = 128
TOKENS = 1024
D = 1024
HEADS = 8
KV_HEADS = 8
HEAD = 128
FF = 3072
LAYERS = 1
THETA = 10000
NAMES = ("wq", "wk", "wv", "wo", "w_gate", "w_up", "w_down")
SHAPES = {
    "wq": (LAYERS, D, HEADS * HEAD),
    "wk": (LAYERS, D, KV_HEADS * HEAD),
    "wv": (LAYERS, D, KV_HEADS * HEAD),
    "wo": (LAYERS, HEADS * HEAD, D),
    "w_gate": (LAYERS, D, FF),
    "w_up": (LAYERS, D, FF),
    "w_down": (LAYERS, FF, D),
}


def bump(key, n, height):
    away = (jnp.arange(n, dtype=jnp.int32) - jax.random.randint(key, (), 0, n, jnp.int32)) % n
    return jnp.where(away < n // 8, height, 1.0)


def together(key, own, strength):
    shared = jax.random.normal(key, own.shape[1:], jnp.float32)
    return (own + strength * shared) * lax.rsqrt(1 + strength * strength)


def setup_inputs(seed: int = 0, part: int = 0) -> dict:
    kx, kdy, ka, kb, kz, kf, kh, kl, *keys = jax.random.split(jax.random.key(seed), 8 + 3 * len(NAMES))
    kx, kdy, ka, kb = (jax.random.fold_in(k, part) for k in (kx, kdy, ka, kb))
    kw, km, kv = (keys[i::3] for i in range(3))
    shape = (SEQUENCES, TOKENS, D)
    much_x, much_dy = jax.random.uniform(kz, (2,), jnp.float32, 0.0, 1.0)
    loud = 2.0 ** jax.random.uniform(jax.random.fold_in(kz, 1), (), jnp.float32, -1.0, 2.0)
    layers = 2.0 ** jax.random.uniform(kl, (LAYERS, 1, 1), jnp.float32, -1.0, 1.0)
    times = {"wq": 1.0, "wk": 1.0, "wv": 2.0, "wo": layers, "w_gate": 1.0, "w_up": bump(kh, FF, 4.0), "w_down": layers}
    x = together(ka, jax.random.normal(kx, shape, jnp.float32), much_x) * bump(kf, D, 4.0)
    dy = together(kb, jax.random.normal(kdy, shape, jnp.float32), much_dy)
    drawn = {"x": x.astype(jnp.bfloat16), "dy": (loud * dy * (SEQUENCES * TOKENS) ** -0.5).astype(jnp.bfloat16)}
    for key, name in zip(kw, NAMES, strict=True):
        drawn[name] = (jax.random.normal(key, SHAPES[name], jnp.float32) * SHAPES[name][1] ** -0.5 * times[name]).astype(jnp.bfloat16)
    return drawn


def matmul(a, w):
    return jnp.dot(a, w, preferred_element_type=jnp.float32).astype(jnp.bfloat16)


def normed(h):
    wide = h.astype(jnp.float32)
    scale = lax.rsqrt(jnp.mean(wide**2, -1, keepdims=True) + 1e-6)
    return (wide * scale).astype(jnp.bfloat16)


def turned(t, theta):
    half = t.shape[-1] // 2
    angle = jnp.arange(t.shape[0], dtype=jnp.float32)[:, None] * theta ** (-jnp.arange(half, dtype=jnp.float32) / half)
    cos, sin = jnp.cos(angle)[:, None], jnp.sin(angle)[:, None]
    a, b = t[..., :half].astype(jnp.float32), t[..., half:].astype(jnp.float32)
    return jnp.concatenate([a * cos - b * sin, b * cos + a * sin], -1).astype(jnp.bfloat16)


def seen_by(q, k, v):
    tokens, kv = q.shape[0], k.shape[1]
    q = q.reshape(tokens, kv, -1, q.shape[-1])
    scores = jnp.einsum("tgsd,ugd->gstu", q.astype(jnp.float32), k.astype(jnp.float32)) * q.shape[-1] ** -0.5
    place = jnp.arange(tokens)
    weights = jax.nn.softmax(jnp.where(place[:, None] >= place, scores, -jnp.inf), -1).astype(jnp.bfloat16)
    return jnp.einsum("gstu,ugd->tgsd", weights.astype(jnp.float32), v.astype(jnp.float32)).astype(jnp.bfloat16).reshape(tokens, -1)


def layer(h, w):
    a = normed(h)
    q, k = (turned(matmul(a, w[name]).reshape(h.shape[0], -1, HEAD), THETA) for name in ("wq", "wk"))
    h = h + matmul(seen_by(q, k, matmul(a, w["wv"]).reshape(h.shape[0], -1, HEAD)), w["wo"])
    b = normed(h)
    gate = jnp.dot(b, w["w_gate"], preferred_element_type=jnp.float32)
    up = jnp.dot(b, w["w_up"], preferred_element_type=jnp.float32)
    return h + matmul((jax.nn.silu(gate) * up).astype(jnp.bfloat16), w["w_down"])


def stack(weights, h):
    return lax.scan(lambda h, w: (layer(h, w), None), h, weights)[0]


def reference(x, dy, wq, wk, wv, wo, w_gate, w_up, w_down):
    weights = dict(zip(NAMES, (wq, wk, wv, wo, w_gate, w_up, w_down), strict=True))

    def take(so_far, sequence):
        h, by_y = sequence
        _, back = jax.vjp(stack, weights, h)
        by_weights, by_h = back(by_y)
        return jax.tree.map(lambda total, term: total + term.astype(jnp.float32), so_far, by_weights), by_h

    none_yet = {name: jnp.zeros(w.shape, jnp.float32) for name, w in weights.items()}
    by_weights, by_x = lax.scan(take, none_yet, (x, dy))
    return (by_x, *(by_weights[name].astype(jnp.bfloat16) for name in NAMES))
```

```python
import functools
import math

import jax
import jax.numpy as jnp
from jax import lax
from jax.experimental import pallas as pl
from jax.experimental.pallas import tpu as pltpu
from jax.sharding import PartitionSpec as P

BF, F32 = jnp.bfloat16, jnp.float32
HIDDEN = -2e30
LOG2E = 1.4426950408889634
VMEM = 63 * 2**20
EPS = 1e-6
HEAD = 128
THETA = 10000
NAMES = ("wq", "wk", "wv", "wo", "w_gate", "w_up", "w_down")
QB = 256
ALL = slice(None)
INSIDE, OUTSIDE = pl.BlockSpec(memory_space=pltpu.VMEM), pl.BlockSpec(memory_space=pl.ANY)


def _loop(first, last, body):
    lax.fori_loop(first, last, lambda b, _: body(b), None)


def _like(*arrays):
    return [jax.ShapeDtypeStruct(a.shape, BF) for a in arrays]


STRIDE = (32, 8, 2)
X, Y, Z = (0, 1, 2), (1, 2, 0), (2, 0, 1)
RING, UP, DOWN = 4, 1, 3


def _place():
    me = lax.axis_index("dp")
    return me, [me // s % RING for s in STRIDE], me % 2


def _peer(me, at, axis, by):
    return me + ((at[axis] + by) % RING - at[axis]) * STRIDE[axis]


def _send(src, dst, send, recv, to):
    c = pltpu.make_async_remote_copy(src_ref=src, dst_ref=dst, send_sem=send, recv_sem=recv, device_id={"dp": to}, device_id_type=pl.DeviceIdType.MESH)
    c.start()
    return c


def _greet():
    me, at, core = _place()
    barrier = pltpu.get_barrier_semaphore()
    peers = [me + 1 - 2 * core] + [_peer(me, at, axis, by) for axis in range(3) for by in (UP, DOWN)]
    for p in peers:
        pl.semaphore_signal(barrier, inc=1, device_id={"dp": p}, device_id_type=pl.DeviceIdType.MESH)
    pl.semaphore_wait(barrier, len(peers))


def _spot(ref, depth, b):
    return (lambda: ref, lambda: ref.at[b], lambda: ref.at[b // RING, b % RING])[depth]()


def _add(terms, dst, depth, spot=None):
    def body(b):
        values = [(spot or _spot)(t, depth, b)[...].astype(F32) for t in terms]
        _spot(dst, depth, b)[...] = functools.reduce(jnp.add, values).astype(BF)

    _loop(0, math.prod(dst.shape[:depth]), body)


class _Scatter:
    def __init__(self, items, ins, outs, sems, rooms, loads, *bufs):
        self.items, self.ins, self.outs, self.sems, self.loads = items, ins, outs, sems, loads
        per = len(bufs) // len(items)
        self.bufs = [bufs[per * i : per * (i + 1)] for i in range(len(items))]
        self.rooms = dict(zip(_kinds(items), rooms))
        self.me, self.at, self.core = _place()
        self.sent, self.flights, self.own = [], {}, {}

    def source(self, i, d, c):
        ref, row, rows, first, cols, axes = self.items[i]
        index = [ALL] * 3
        index[axes[0]] = (self.at[axes[0]] + d) % RING
        return self.ins[ref].at[(*index, c, pl.ds(row, rows), pl.ds(first, cols))]

    def pair(self, i, k, slot):
        return self.sems.at[i, k, 0, slot], self.sems.at[i, k, 1, slot]

    def begin(self, i):
        for d in (2, UP, DOWN, 0):
            c = _send(self.source(i, d, 1 - self.core), self.bufs[i][0].at[d], *self.pair(i, 0, d), self.me + 1 - 2 * self.core)
            self.flights[i, 0, d] = c
            self.sent.append(c)
        self.fetch(i, 2)

    def fetch(self, i, d):
        room = self.rooms[_kind(self.items[i])] if d in (UP, 0) else self.bufs[i][4]
        self.own[i, d] = room, pltpu.make_async_copy(self.source(i, d, self.core), room, self.loads.at[i, d])
        self.own[i, d][1].start()

    def merge(self, i):
        acc = self.bufs[i][0]
        self.fetch(i, UP)
        for d, ahead in ((2, DOWN), (UP, 0), (DOWN, None), (0, None)):
            self.flights[i, 0, d].wait_recv()
            room, load = self.own[i, d]
            load.wait()
            _add([acc.at[d], room], acc.at[d], 2)
            if ahead is not None:
                self.fetch(i, ahead)
            if d == 2:
                self.first_out(i, 1)
            if d == DOWN:
                self.second_out(i, 1)

    def half(self, i, k, ref, h):
        if k < 3:
            return ref.at[pl.ds(2 * h, 2)]
        n = self.items[i][4] // 2
        return ref.at[:, pl.ds(h * n, n)]

    def post(self, i, k, slot, src, dst, by):
        c = _send(src, dst, *self.pair(i, k, slot), _peer(self.me, self.at, self.items[i][5][k - 1], by))
        self.flights[i, k, slot] = c
        self.sent.append(c)

    def phase(self, i, k):
        return self.bufs[i][4 * k - 4 : 4 * k]

    def first_out(self, i, k):
        acc, early, low, high = self.phase(i, k)
        for slot, by in enumerate((UP, DOWN)):
            self.post(i, k, slot, self.half(i, k, acc.at[2], slot), early.at[slot], by)

    def second_out(self, i, k):
        acc, early, low, high = self.phase(i, k)
        for slot, by, h, land in ((2, UP, 1, low), (3, DOWN, 0, high)):
            self.post(i, k, slot, self.half(i, k, acc.at[by], h), self.half(i, k, land, h), by)

    def relay(self, i, k):
        acc, early, low, high = self.phase(i, k)
        for slot, d, land in ((0, UP, low), (1, DOWN, high)):
            self.flights[i, k, slot].wait_recv()
            part = self.half(i, k, acc.at[d], slot)
            _add([part, early.at[slot]], part, 3 - k)
            self.post(i, k, 4 + slot, part, self.half(i, k, land, slot), d)

    def finish(self, i, k):
        acc, early, low, high = self.phase(i, k)
        for slot in (2, 3, 4, 5):
            self.flights[i, k, slot].wait_recv()
        *_, (_, second, third) = self.items[i]

        def shifted(ref, depth, b):
            s, t = (self.at[second] + b // RING) % RING, (self.at[third] + b % RING) % RING
            return ref.at[(s, t) if second < third else (t, s)]

        _add([acc.at[0], low, high], self.outs[i] if k == 3 else self.bufs[i][4 * k], 3 - k, shifted if k == 1 else None)
        if k < 3:
            self.first_out(i, k + 1)
            self.second_out(i, k + 1)

    def steps(self, every):
        return [functools.partial(f, i, k) for k in (1, 2, 3) for f in (self.relay, self.finish) for i in every]

    def end(self):
        for c in self.sent:
            c.wait_send()


def _kind(item):
    return item[2], item[4]


def _kinds(items):
    return sorted(set(map(_kind, items)))


def _scatter_scratch(items):
    def room(*shape):
        return pltpu.VMEM(shape, BF)

    scratch = []
    for kind in map(_kind, items):
        for ring in ((RING, RING), (RING,)):
            scratch += [room(RING, *ring, *kind), room(2, 2, *ring[1:], *kind), room(*ring, *kind), room(*ring, *kind)]
        r, n = kind
        scratch += [room(RING, *kind), room(2, r, n // 2), room(*kind), room(*kind)]
    return [pltpu.SemaphoreType.DMA((len(items), 4, 2, 6)), [room(RING, RING, *kind) for kind in _kinds(items)],
            pltpu.SemaphoreType.DMA((len(items), RING)), *scratch]


def _cut(shape):
    return RING, RING, RING, 2, shape[0] // 128, shape[1]


class _Gather:
    def __init__(self, axes, ins, outs, sems, local):
        self.axes, self.ins, self.outs, self.sems, self.local = axes, ins, outs, sems, local
        self.me, self.at, self.core = _place()
        self.sent, self.flights, self.mine = [], {}, {}

    def region(self, i, full, by=None, part=None):
        index = [ALL if a in full else self.at[a] for a in range(3)]
        if by is not None:
            axis, d = by
            index[axis] = (self.at[axis] + d) % RING
        tail = ALL
        if part is not None and full:
            index[full[0]] = pl.ds(2 * part, 2)
        elif part is not None:
            w = self.outs[i].shape[-1] // 2
            tail = pl.ds(part * w, w)
        return self.outs[i].at[(*index, self.core, ALL, tail)]

    def post(self, i, k, slot, src, dst, to):
        c = _send(src, dst, self.sems.at[i, k, 0, slot], self.sems.at[i, k, 1, slot], to)
        self.flights[i, k, slot] = c
        self.sent.append(c)

    def along(self, i, k):
        axis = self.axes[i][k]
        return axis, self.axes[i][:k], *[_peer(self.me, self.at, axis, by) for by in (UP, DOWN)]

    def start(self, i, k):
        axis, full, up, down = self.along(i, k)
        for slot, part, to in ((0, 0, up), (1, 1, down), (2, 1, up), (3, 0, down)):
            there = here = self.region(i, full, None, part)
            if k == 0:
                w = self.ins[i].shape[-1] // 2
                here = self.ins[i].at[:, pl.ds(part * w, w)]
            self.post(i, k, slot, here, there, to)
        if k == 0:
            self.mine[i] = pltpu.make_async_copy(self.ins[i], self.region(i, ()), self.local.at[i])
            self.mine[i].start()
        if k == 2:
            self.across(i, 0, 0)

    def across(self, i, slot, by):
        axis, full, _, _ = self.along(i, 2)
        piece = self.region(i, full, (axis, by))
        self.post(i, 3, slot, piece, piece, self.me + 1 - 2 * self.core)

    def relay(self, i, k):
        axis, full, up, down = self.along(i, k)
        for slot, by, to in ((0, DOWN, up), (1, UP, down)):
            self.flights[i, k, slot].wait_recv()
            piece = self.region(i, full, (axis, by), slot)
            self.post(i, k, 4 + slot, piece, piece, to)

    def finish(self, i, k):
        for slot in (2, 3):
            self.flights[i, k, slot].wait_recv()
        if k == 0:
            self.mine[i].wait()
        if k == 2:
            self.across(i, 1, UP)
            self.across(i, 2, DOWN)
        for slot in (4, 5):
            self.flights[i, k, slot].wait_recv()
        if k == 2:
            self.across(i, 3, 2)
        else:
            self.start(i, k + 1)

    def arrive(self, i):
        for slot in range(4):
            self.flights[i, 3, slot].wait_recv()

    def end(self):
        for c in self.sent:
            c.wait_send()


def _interleave(work, steps, lead):
    done = 0
    for n, f in enumerate(work):
        f()
        upto = max(n + 1 - lead, 0) * len(steps) // (len(work) - lead)
        for s in steps[done:upto]:
            s()
        done = upto


def _dot(a, b, ca, cb):
    return lax.dot_general(a, b, (((ca,), (cb,)), ((), ())), preferred_element_type=F32)


def _cols(n, width):
    return pl.ds(pl.multiple_of(n * width, width), width)


def _turn(t, cos, sin):
    return t * cos + pltpu.roll(t, HEAD // 2, 1) * sin


def _scores(k, q, first):
    n = k.shape[0] - first
    low = lax.broadcasted_iota(jnp.int32, (n, q.shape[0]), 0) <= lax.broadcasted_iota(jnp.int32, (n, q.shape[0]), 1)
    diagonal = jnp.where(low, _dot(k[first:], q, 1, 1), HIDDEN)
    return ([_dot(k[:first], q, 1, 1)] if first else []) + [diagonal]


def _attend(h, q_ref, k_ref, v_ref, o_ref, lse_ref):
    here = _cols(h, HEAD)
    e = HEAD**-0.5 * LOG2E
    tokens = q_ref.shape[0]
    k, vt = k_ref[:, here], v_ref[:, here].T
    vt = jnp.concatenate([vt, jnp.ones((16, tokens), BF)], axis=0)
    for at in range(0, tokens, QB):
        parts = _scores(k[: at + QB], q_ref[at : at + QB, here], at)
        top = functools.reduce(jnp.maximum, [s.max(axis=0, keepdims=True) for s in parts])
        p = jnp.concatenate([jnp.exp2((s - top) * e).astype(BF) for s in parts], axis=0)
        mix = _dot(vt[:, : at + QB], p, 1, 0)
        total = mix[HEAD : HEAD + 1]
        o_ref[at : at + QB, here] = (mix[:HEAD] * (1 / total)).T.astype(BF)
        lse_ref[pl.ds(h, 1), at : at + QB] = top * e + jnp.log(total) * LOG2E


LANES = (2, 1, 0), (0, 2, 1), (1, 0, 2)


def _front_kernel(*refs):
    x, cos, sin, shards, q, k, v, o, lse, whole, kept, a, wide, sems, local, keep = refs
    g = _Gather((*LANES, X, *LANES), shards, (*wide, *whole), sems, local)
    _greet()
    every, first, later = range(7), range(3), range(3, 7)
    for i in every:
        g.start(i, 0)

    def norm(b):
        rows = pl.ds(b * HEAD, HEAD)
        h = x[rows, :].astype(F32)
        a[rows, :] = (h * lax.rsqrt(jnp.mean(h * h, 1, keepdims=True) + EPS)).astype(BF)

    _loop(0, x.shape[0] // HEAD, norm)
    for n in range(2):
        for i in every:
            g.relay(i, n)
        for i in every:
            g.finish(i, n)
    for i in first:
        g.relay(i, 2)
    for i in first:
        g.finish(i, 2)

    copies = []

    def project(i, out):
        g.arrive(i)
        w = wide[i].reshape(x.shape)
        copies.append(pltpu.make_async_copy(wide[i], kept[i], keep.at[i]))
        copies[-1].start()

        def cols(n):
            t = jnp.dot(a[...], w[:, _cols(n, QB)], preferred_element_type=F32).astype(BF)
            for j in range(QB // HEAD):
                part = t[:, j * HEAD : (j + 1) * HEAD]
                if out is not v:
                    part = _turn(part.astype(F32), cos[...], sin[...]).astype(BF)
                out[:, _cols(n * (QB // HEAD) + j, HEAD)] = part

        _loop(0, x.shape[1] // QB, cols)

    def heads(n):
        _loop(n, n + 2, lambda h: _attend(h, q, k, v, o, lse))

    work = [functools.partial(project, i, out) for i, out in enumerate((q, k, v))]
    work += [functools.partial(heads, n) for n in range(0, 8, 2)]
    steps = [functools.partial(g.relay, i, 2) for i in later] + [functools.partial(g.finish, i, 2) for i in later]
    _interleave(work, steps, 2)
    for i in later:
        g.arrive(i)
    for c in copies:
        c.wait()
    g.end()


def _call(kernel, number, scratch, ins, out_shape, in_specs, out_specs):
    return pl.pallas_call(
        kernel,
        out_shape=out_shape,
        in_specs=in_specs,
        out_specs=out_specs,
        scratch_shapes=scratch,
        compiler_params=pltpu.CompilerParams(collective_id=number, has_side_effects=True, vmem_limit_bytes=VMEM),
    )(*ins)


def front(x, cos, sin, shards):
    square, many = _like(x), len(shards)
    spread = [jax.ShapeDtypeStruct(_cut((s.shape[0] * 128, s.shape[1])), BF) for s in shards]
    lse = jax.ShapeDtypeStruct((x.shape[1] // HEAD, x.shape[0]), F32)
    dma = pltpu.SemaphoreType.DMA
    *seen, lse, late, early = _call(
        _front_kernel, 0, [pltpu.VMEM(x.shape, BF), [pltpu.VMEM(s.shape, BF) for s in spread[:3]], dma((many, 4, 2, 6)), dma((many,)), dma((3,))],
        (x, cos, sin, shards), (*square * 4, lse, spread[3:], spread[:3]),
        (INSIDE, INSIDE, INSIDE, [INSIDE] * many), (INSIDE, INSIDE, INSIDE, INSIDE, INSIDE, [OUTSIDE] * 4, [OUTSIDE] * 3))
    return seen, lse, [w.reshape(-1, w.shape[-1]) for w in (*early, *late)]


def _attend_back(h, q_ref, k_ref, v_ref, do_ref, lse_ref, delta_ref, dk_s, dv_s, cos, sin):
    here = _cols(h, HEAD)
    scale = HEAD**-0.5
    tokens = q_ref.shape[0]
    k, v = k_ref[:, here], v_ref[:, here]
    kt = k.T
    for at in reversed(range(0, tokens, QB)):
        n = at + QB
        rows = slice(at, n)
        q, do = q_ref[rows, here], do_ref[rows, here]
        lse, delta = lse_ref[pl.ds(h, 1), rows], delta_ref[pl.ds(h, 1), rows]
        dp = _dot(v[:n], do, 1, 1)
        p = jnp.concatenate([jnp.exp2(s * (scale * LOG2E) - lse) for s in _scores(k[:n], q, at)], axis=0)
        ds = (p * (dp - delta)).astype(BF)
        by_v, by_k = _dot(p.astype(BF), do, 1, 0), _dot(ds, q, 1, 0)
        if n == tokens:
            dv_s[...] = by_v
            dk_s[...] = by_k
        else:
            dv_s[:n] += by_v
            dk_s[:n] += by_k
        dq = (_dot(kt[:, :n], ds, 1, 0) * scale).T.astype(BF)
        q_ref[rows, here] = _turn(dq.astype(F32), cos[rows], -sin[rows]).astype(BF)
    dk = (dk_s[...] * scale).astype(BF)
    k_ref[:, here] = _turn(dk.astype(F32), cos[...], -sin[...]).astype(BF)
    v_ref[:, here] = dv_s[...].astype(BF)


def _norm_back(h, by_b):
    r = lax.rsqrt(jnp.mean(h * h, -1, keepdims=True) + EPS)
    return r * by_b - h * (r * r * r * jnp.mean(h * by_b, -1, keepdims=True))


def _plus(h, by_h):
    return (h.astype(F32) + by_h.astype(BF).astype(F32)).astype(BF)


def _normed(h):
    h = h.astype(F32)
    return (h * lax.rsqrt(jnp.mean(h * h, -1, keepdims=True) + EPS)).astype(BF)


def _middle_kernel(blocks, *refs):
    h, dy, gate_cols, up_cols, down_rows, gate_rows, up_rows, dh, by_gate, by_up, by_down, b, bt, d_gate, d_up, db = refs
    step = pl.program_id(0)
    tokens, width = h.shape[0], by_gate.shape[1]

    @pl.when(step == 0)
    def _():
        def norm(n):
            rows = pl.ds(pl.multiple_of(n * HEAD, HEAD), HEAD)
            b[rows, :] = _normed(h[rows, :])
            bt[:, rows] = b[rows, :].T

        _loop(0, tokens // HEAD, norm)

    @pl.when(step < blocks)
    def _():
        here = _cols(step, width)
        acts = []
        for at in range(0, tokens, ROWS):
            rows = slice(at, at + ROWS)
            gate, up = _dot(b[rows, :], gate_cols[...], 1, 0), _dot(b[rows, :], up_cols[...], 1, 0)
            by_act = _dot(dy[rows, :], down_rows[...], 1, 1).astype(BF).astype(F32)
            share = lax.logistic(gate)
            silu = gate * share
            acts.append((silu * up).astype(BF))
            d_up[rows, here] = (by_act * silu).astype(BF)
            d_gate[rows, here] = (by_act * up * (share + silu * (1 - share))).astype(BF)
        by_down[...] = _dot(jnp.concatenate([a.T for a in acts], axis=1), dy[...], 1, 0).astype(BF)
        by_gate[...] = _dot(bt[...], d_gate[:, here], 1, 0).astype(BF)
        by_up[...] = _dot(bt[...], d_up[:, here], 1, 0).astype(BF)

    @pl.when(step >= blocks)
    def _():
        db[:, _cols(step - blocks, QB)] = _dot(d_gate[...], gate_rows[...], 1, 1) + _dot(d_up[...], up_rows[...], 1, 1)

    @pl.when(step == pl.num_programs(0) - 1)
    def _():
        def norm(n):
            rows = pl.ds(pl.multiple_of(n * HEAD, HEAD), HEAD)
            dh[rows, :] = _plus(dy[rows, :], _norm_back(h[rows, :].astype(F32), db[rows, :]))

        _loop(0, tokens // HEAD, norm)


ROWS, WIDTH = 512, 256


def middle(h, dy, w_gate, w_up, w_down):
    (tokens, d), ff = h.shape, w_gate.shape[1]
    blocks, more = ff // WIDTH, d // QB
    fixed = pl.BlockSpec((tokens, d), lambda s: (0, 0))
    cols = pl.BlockSpec((d, WIDTH), lambda s: (0, jnp.minimum(s, blocks - 1)))
    rows = pl.BlockSpec((WIDTH, d), lambda s: (jnp.minimum(s, blocks - 1), 0))
    across = pl.BlockSpec((QB, ff), lambda s: (jnp.maximum(s - blocks, 0), 0))
    square, wide = pltpu.VMEM(h.shape, BF), pltpu.VMEM((tokens, ff), BF)
    return pl.pallas_call(
        functools.partial(_middle_kernel, blocks),
        grid=(blocks + more,),
        out_shape=_like(h, w_gate, w_up, w_down),
        in_specs=[fixed, fixed, cols, cols, rows, across, across],
        out_specs=[fixed, cols, cols, rows],
        scratch_shapes=[square, square, wide, wide, pltpu.VMEM(h.shape, F32)],
        compiler_params=pltpu.CompilerParams(dimension_semantics=("arbitrary",), vmem_limit_bytes=VMEM),
    )(h, dy, w_gate, w_up, w_down, w_gate, w_up)


def _back_kernel(items, *refs):
    x, cos, sin, dh, lse, far, weights, terms, dx, grads, mine, near, w, at, stage, delta, dk_s, dv_s, load, store, scratch = refs
    s = _Scatter(items, (*terms, *grads), mine, *scratch)
    q, k, v, o = near
    tokens, d = x.shape
    _greet()
    early, late = [i for i in range(len(items)) if items[i][0] < 3 or items[i][0] == 6], range(3, 6)
    for i in range(3):
        s.begin(i)
    wq, wk, wv, wo = weights
    pairs = [(far[3], o), (wo, w.at[0]), *zip(far, (q, k, v)), (wk, w.at[1]), (wv, w.at[2]), (wq, w.at[0])]
    loads = [pltpu.make_async_copy(src, dst, load.at[n]) for n, (src, dst) in enumerate(pairs)]
    get_o, get_wo, *get_qkv, get_wk, get_wv, get_wq = loads
    for c in loads[:-1]:
        c.start()
    flat = [g.reshape(d, d) for g in grads]
    stores = [pltpu.make_async_copy(src, dst, store.at[n]) for n, (src, dst) in enumerate(zip((o, stage, o, stage), flat))]
    put_q, put_k, put_v, put_o = stores

    def transposed():
        def body(n):
            at[:, _cols(n, HEAD)] = _normed(x[pl.ds(n * HEAD, HEAD), :]).T

        _loop(0, tokens // HEAD, body)
        get_o.wait()

    def by_wo(n):
        stage[pl.ds(n * QB, QB), :] = _dot(o[:, _cols(n, QB)].T, dh[...], 1, 0).astype(BF)

    def wo_done():
        put_o.start()
        get_wo.wait()

    def by_o(n):
        do = _dot(dh[...], w[0, pl.ds(n * QB, QB), :], 1, 1).astype(BF)
        for j in range(QB // HEAD):
            h = n * (QB // HEAD) + j
            here, part = _cols(h, HEAD), do[:, j * HEAD : (j + 1) * HEAD]
            product = part.astype(F32) * o[:, here].astype(F32)
            delta[pl.ds(h, 1), :] = product.T.sum(axis=0, keepdims=True)
            o[:, here] = part

    def o_begun():
        put_o.wait()
        for i in early[3:]:
            s.begin(i)

    def o_done():
        for c in get_qkv:
            c.wait()
        get_wq.start()

    def head(h):
        _attend_back(h, q, k, v, o, lse, delta, dk_s, dv_s, cos, sin)

    def by_weight(i, into, put):
        def body(n):
            here = _cols(n, QB)
            into[:, here] = jnp.dot(at[...], near[i][:, here], preferred_element_type=F32).astype(BF)

        _loop(0, d // QB, body)
        put.start()

    def weight_done(i, put):
        put.wait()
        s.begin(3 + i)

    def by_x(b):
        rows = pl.ds(b * QB, QB)
        da = _dot(q[rows, :], w[0], 1, 1) + _dot(k[rows, :], w[1], 1, 1) + _dot(v[rows, :], w[2], 1, 1)
        dx[rows, :] = _plus(dh[rows, :], _norm_back(x[rows, :].astype(F32), da))

    def part(body, n):
        return functools.partial(_loop, n, n + 2, body)

    work = [transposed, part(by_wo, 0), part(by_wo, 2), wo_done, part(by_o, 0), o_begun, part(by_o, 2), o_done]
    work += [part(head, n) for n in range(0, 8, 2)]
    def do(steps):
        for f in steps:
            f()

    steps, n = s.steps(early), len(early)
    merges = [functools.partial(s.merge, i) for i in early]
    _interleave(work, merges[:3] + steps[:3] + merges[3:] + steps[3 : 2 * n], 2)
    steps = steps[2 * n :]
    by_weight(0, o, put_q)
    do(steps[:3])
    by_weight(1, stage, put_k)
    weight_done(0, put_q)
    do(steps[3:n])
    by_weight(2, o, put_v)
    weight_done(1, put_k)
    do(steps[n : n + 3])
    do([get_wk.wait, get_wv.wait, get_wq.wait])
    by_x(0)
    weight_done(2, put_v)
    s.merge(3)
    do(steps[n + 3 : 2 * n])
    by_x(1)
    s.merge(4)
    do(steps[2 * n : 3 * n])
    by_x(2)
    s.merge(5)
    last_steps, m = s.steps(late), len(late)
    do(last_steps[:m])
    by_x(3)
    do(steps[3 * n :] + last_steps[m:])
    s.end()


def back(x, cos, sin, dh, lse, seen, weights, terms):
    d = x.shape[1]
    items = [(0, 0, 8, 0, 3 * d, X), (1, 0, 8, 0, 3 * d, Y), (2, 0, 24, 0, d, Z), *((3 + n, 0, 8, 0, d, axes) for n, axes in enumerate((X, Y, Z))),
             *((6, 0, 8, n * d // 2, d // 2, axes) for n, axes in enumerate((X, Y)))]
    square, column, dma = pltpu.VMEM(x.shape, BF), pltpu.VMEM((x.shape[0], HEAD), F32), pltpu.SemaphoreType.DMA
    blocks = [jax.ShapeDtypeStruct((item[2], item[4]), BF) for item in items]
    dx, _, (gate, up, down, *four) = _call(
        functools.partial(_back_kernel, items), 1,
        [[square] * 4, pltpu.VMEM((3, *x.shape), BF), square, square, pltpu.VMEM(lse.shape, F32), column, column, dma((8,)), dma((4,)), _scatter_scratch(items)],
        (x, cos, sin, dh, lse, seen, weights, [t.reshape(_cut(t.shape)) for t in terms]),
        (*_like(x), [jax.ShapeDtypeStruct(_cut(x.shape), BF)] * 4, blocks),
        (INSIDE, INSIDE, INSIDE, INSIDE, INSIDE, [OUTSIDE] * 4, [OUTSIDE] * 4, [OUTSIDE] * 3), (INSIDE, [OUTSIDE] * 4, [INSIDE] * len(items)))
    return dx, (*four, gate, up, down)


def _last_kernel(dx_in, q, k, v, left, right, gate, up, down, dx, *outs):
    dx[0] = dx_in[...]
    for out, ref in zip((*outs[:3], *outs[4:]), (q, k, v, gate, up, down)):
        out[0] = ref[...]
    half = left.shape[1]
    outs[3][0, :, :half] = left[...]
    outs[3][0, :, half:] = right[...]


def last(dx, blocks, shapes):
    return pl.pallas_call(_last_kernel, out_shape=[jax.ShapeDtypeStruct(s, BF) for s in shapes], in_specs=[INSIDE] * (1 + len(blocks)),
                          out_specs=[INSIDE] * len(shapes))(dx, *blocks)


def solution(mesh):
    def step(x, dy, *weights):
        shapes = [a.shape for a in (x, *weights)]
        x, dy = x[0], dy[0]
        half = HEAD // 2
        angle = jnp.arange(x.shape[0], dtype=F32)[:, None] * THETA ** (-jnp.arange(half, dtype=F32) / half)
        cos, sin = jnp.cos(angle), jnp.sin(angle)
        cos, sin = jnp.concatenate([cos, cos], 1), jnp.concatenate([-sin, sin], 1)
        seen, lse, whole = front(x, cos, sin, [w[0] for w in weights])
        wo = whole[3]
        h = x + jnp.dot(seen[3], wo, preferred_element_type=F32).astype(BF)
        dh, *terms = middle(h, dy, *whole[4:])
        dx, blocks = back(x, cos, sin, dh, lse, seen, whole[:4], terms)
        return tuple(last(dx, blocks, shapes))

    states, cut = P(("rep", "dp"), None, None), P(None, "dp", None)
    return jax.shard_map(
        step,
        mesh=mesh,
        in_specs=(states, states) + (cut,) * 7,
        out_specs=(states,) + (P("rep", "dp", None),) * 7,
        check_vma=False,
    )
```

```python
import functools
import math

import jax
import jax.numpy as jnp
import numpy as np
from jax import lax
from jax.experimental import pallas as pl
from jax.experimental.pallas import tpu as pltpu
from jax.sharding import PartitionSpec as P

BF, F32 = jnp.bfloat16, jnp.float32
HIDDEN = -2e30
LOG2E = 1.4426950408889634
VMEM = 63 * 2**20
EPS = 1e-6
HEAD = 128
THETA = 10000
NAMES = ("wq", "wk", "wv", "wo", "w_gate", "w_up", "w_down")
QB = 256
ALL = slice(None)
INSIDE, OUTSIDE = pl.BlockSpec(memory_space=pltpu.VMEM), pl.BlockSpec(memory_space=pl.ANY)


def _loop(first, last, body):
    lax.fori_loop(first, last, lambda b, _: body(b), None)


def _like(*arrays):
    return [jax.ShapeDtypeStruct(a.shape, BF) for a in arrays]


STRIDE = (32, 8, 2)
X, Y, Z = (0, 1, 2), (1, 2, 0), (2, 0, 1)
RING, UP, DOWN = 4, 1, 3
ORDER = 2, UP, DOWN, 0


def _place():
    me = lax.axis_index("dp")
    return me, [me // s % RING for s in STRIDE], me % 2


def _peer(me, at, axis, by):
    return me + ((at[axis] + by) % RING - at[axis]) * STRIDE[axis]


def _send(src, dst, send, recv, to):
    c = pltpu.make_async_remote_copy(src_ref=src, dst_ref=dst, send_sem=send, recv_sem=recv, device_id={"dp": to}, device_id_type=pl.DeviceIdType.MESH)
    c.start()
    return c


def _greet():
    me, at, core = _place()
    barrier = pltpu.get_barrier_semaphore()
    peers = [me + 1 - 2 * core] + [_peer(me, at, axis, by) for axis in range(3) for by in (UP, 2, DOWN)]
    for p in peers:
        pl.semaphore_signal(barrier, inc=1, device_id={"dp": p}, device_id_type=pl.DeviceIdType.MESH)
    pl.semaphore_wait(barrier, len(peers))


def _spot(ref, depth, b):
    return (lambda: ref, lambda: ref.at[b], lambda: ref.at[b // RING, b % RING])[depth]()


def _add(terms, dst, depth, spot=None):
    def body(b):
        values = [(spot or _spot)(t, depth, b)[...].astype(F32) for t in terms]
        _spot(dst, depth, b)[...] = functools.reduce(jnp.add, values).astype(BF)

    _loop(0, math.prod(dst.shape[:depth]), body)


class _Scatter:
    def __init__(self, items, ins, outs, sems, loads, *bufs):
        self.items, self.ins, self.outs, self.sems, self.loads = items, ins, outs, sems, loads
        per = len(bufs) // len(items)
        self.bufs = [bufs[per * i : per * (i + 1)] for i in range(len(items))]
        self.me, self.at, self.core = _place()
        self.sent, self.flights, self.own = [], {}, {}

    def source(self, i, d, c):
        ref, row, rows, first, cols, axes = self.items[i]
        index = [ALL] * 3
        index[axes[0]] = (self.at[axes[0]] + d) % RING
        return self.ins[ref].at[(*index, c, pl.ds(row, rows), pl.ds(first, cols))]

    def pair(self, i, k, slot):
        return self.sems.at[i, k, 0, slot], self.sems.at[i, k, 1, slot]

    def begin(self, *some):
        for d in ORDER:
            for i in some:
                c = _send(self.source(i, d, 1 - self.core), self.bufs[i][0].at[d], *self.pair(i, 0, d), self.me + 1 - 2 * self.core)
                self.flights[i, 0, d] = c
                self.sent.append(c)
                if d == 2 or _little(_kind(self.items[i])):
                    self.fetch(i, d)

    def fetch(self, i, d):
        room = self.bufs[i][-1].at[d] if _little(_kind(self.items[i])) else self.bufs[i][4]
        self.own[i, d] = room, pltpu.make_async_copy(self.source(i, d, self.core), room, self.loads.at[i, d])
        self.own[i, d][1].start()

    def merge(self, d, *some):
        for i in some:
            acc = self.bufs[i][0].at[d]
            self.flights[i, 0, d].wait_recv()
            room, load = self.own[i, d]
            load.wait()
            _add([acc, room], acc, 2)
            if d == 2:
                self.first_out(i, 1)
            if d == DOWN:
                self.second_out(i, 1)
            if d and not _little(_kind(self.items[i])):
                self.fetch(i, ORDER[ORDER.index(d) + 1])

    def half(self, i, k, ref, h):
        return ref.at[pl.ds(2 * h, 2)]

    def post(self, i, k, slot, src, dst, by):
        c = _send(src, dst, *self.pair(i, k, slot), _peer(self.me, self.at, self.items[i][5][k - 1], by))
        self.flights[i, k, slot] = c
        self.sent.append(c)

    def phase(self, i, k):
        return self.bufs[i][4 * k - 4 : 4 * k]

    def first_out(self, i, k):
        acc, early, low, high = self.phase(i, k)
        if k == 3:
            self.post(i, k, 0, acc.at[2], early, 2)
            self.post(i, k, 2, acc.at[UP], low, UP)
            self.post(i, k, 3, acc.at[DOWN], high, DOWN)
            return
        for slot, by in enumerate((UP, DOWN)):
            self.post(i, k, slot, self.half(i, k, acc.at[2], slot), early.at[slot], by)

    def second_out(self, i, k):
        acc, early, low, high = self.phase(i, k)
        for slot, by, h, land in ((2, UP, 1, low), (3, DOWN, 0, high)):
            self.post(i, k, slot, self.half(i, k, acc.at[by], h), self.half(i, k, land, h), by)

    def relay(self, i, k):
        acc, early, low, high = self.phase(i, k)
        for slot, d, land in ((0, UP, low), (1, DOWN, high)):
            self.flights[i, k, slot].wait_recv()
            part = self.half(i, k, acc.at[d], slot)
            _add([part, early.at[slot]], part, 3 - k)
            self.post(i, k, 4 + slot, part, self.half(i, k, land, slot), d)

    def finish(self, i, k):
        acc, early, low, high = self.phase(i, k)
        for slot in (0, 2, 3) if k == 3 else (2, 3, 4, 5):
            self.flights[i, k, slot].wait_recv()
        *_, (_, second, third) = self.items[i]

        def shifted(ref, depth, b):
            s, t = (self.at[second] + b // RING) % RING, (self.at[third] + b % RING) % RING
            return ref.at[(s, t) if second < third else (t, s)]

        terms = [acc.at[0], low, high, early]
        _add(terms if k == 3 else terms[:3], self.outs[i] if k == 3 else self.bufs[i][4 * k], 3 - k, shifted if k == 1 else None)
        if k < 3:
            self.first_out(i, k + 1)
        if k < 2:
            self.second_out(i, k + 1)

    def end(self):
        for c in self.sent:
            c.wait_send()


def _little(kind):
    return math.prod(kind) <= 8 * 1024


def _kind(item):
    return item[2], item[4]


def _scatter_scratch(items):
    def room(*shape):
        return pltpu.VMEM(shape, BF)

    scratch = []
    for kind in map(_kind, items):
        for ring in ((RING, RING), (RING,)):
            scratch += [room(RING, *ring, *kind), room(2, 2, *ring[1:], *kind), room(*ring, *kind), room(*ring, *kind)]
        scratch += [room(RING, *kind), room(*kind), room(*kind), room(*kind), room(*((RING,) * 3 if _little(kind) else ()), *kind)]
    return [pltpu.SemaphoreType.DMA((len(items), 4, 2, 6)), pltpu.SemaphoreType.DMA((len(items), RING)), *scratch]


def _cut(shape):
    return RING, RING, RING, 2, shape[0] // 128, shape[1]


class _Gather:
    def __init__(self, items, ins, outs, sems, local):
        self.items, self.ins, self.outs, self.sems, self.local = items, ins, outs, sems, local
        self.me, self.at, self.core = _place()
        self.sent, self.flights, self.mine = [], {}, {}

    def region(self, i, full, by=None, part=None):
        index = [ALL if a in full else self.at[a] for a in range(3)]
        if by is not None:
            axis, d = by
            index[axis] = (self.at[axis] + d) % RING
        ref = self.items[i][0]
        if part is not None and full:
            index[full[0]] = pl.ds(2 * part, 2)
            part = None
        return self.outs[ref].at[(*index, self.core, ALL, self.columns(i, part))]

    def columns(self, i, part):
        _, first, width, _ = self.items[i]
        half = width // 2
        return pl.ds(first, width) if part is None else pl.ds(first + part * half, half)

    def own(self, i, part):
        return self.ins[self.items[i][0]].at[:, self.columns(i, part)]

    def post(self, i, k, slot, src, dst, to):
        c = _send(src, dst, self.sems.at[i, k, 0, slot], self.sems.at[i, k, 1, slot], to)
        self.flights[i, k, slot] = c
        self.sent.append(c)

    def short(self, i, k):
        return k == 0 or k == 1 and self.items[i][0] < 3

    def along(self, i, k):
        *_, axes = self.items[i]
        axis = axes[k]
        return axis, axes[:k], *[_peer(self.me, self.at, axis, by) for by in (UP, DOWN)]

    def start(self, i, k):
        axis, full, up, down = self.along(i, k)
        plan = (0, 0, up), (1, 1, down), (2, 1, up), (3, 0, down)
        if self.short(i, k):
            plan = (2, None, up), (3, None, down), (4, None, _peer(self.me, self.at, axis, 2))
        for slot, part, to in plan:
            there = self.region(i, full, None, part)
            self.post(i, k, slot, there if k else self.own(i, part), there, to)
        if k == 0:
            self.mine[i] = pltpu.make_async_copy(self.own(i, None), self.region(i, ()), self.local.at[i])
            self.mine[i].start()
        if k == 2:
            self.across(i, 0, 0)

    def across(self, i, slot, by):
        axis, full, _, _ = self.along(i, 2)
        piece = self.region(i, full, (axis, by))
        self.post(i, 3, slot, piece, piece, self.me + 1 - 2 * self.core)

    def relay(self, i, k):
        axis, full, up, down = self.along(i, k)
        if self.short(i, k):
            return
        for slot, by, to in ((0, DOWN, up), (1, UP, down)):
            self.flights[i, k, slot].wait_recv()
            piece = self.region(i, full, (axis, by), slot)
            self.post(i, k, 4 + slot, piece, piece, to)

    def finish(self, i, k):
        for slot in (2, 3):
            self.flights[i, k, slot].wait_recv()
        if k == 0:
            self.mine[i].wait()
        if k == 2:
            self.across(i, 1, UP)
            self.across(i, 2, DOWN)
        for slot in (4,) if self.short(i, k) else (4, 5):
            self.flights[i, k, slot].wait_recv()
        if k == 2:
            self.across(i, 3, 2)
        else:
            self.start(i, k + 1)

    def arrive(self, i):
        for slot in range(4):
            self.flights[i, 3, slot].wait_recv()

    def end(self):
        for c in self.sent:
            c.wait_send()


def _dot(a, b, ca, cb):
    return lax.dot_general(a, b, (((ca,), (cb,)), ((), ())), preferred_element_type=F32)


def _cols(n, width):
    return pl.ds(pl.multiple_of(n * width, width), width)


def _turn(t, cos, sin):
    return t * cos + pltpu.roll(t, HEAD // 2, 1) * sin


def _scores(k, q, first):
    n = k.shape[0] - first
    low = lax.broadcasted_iota(jnp.int32, (n, q.shape[0]), 0) <= lax.broadcasted_iota(jnp.int32, (n, q.shape[0]), 1)
    diagonal = jnp.where(low, _dot(k[first:], q, 1, 1), HIDDEN)
    return ([_dot(k[:first], q, 1, 1)] if first else []) + [diagonal]


def _attend(h, q_ref, k_ref, v_ref, o_ref, lse_ref):
    here = _cols(h, HEAD)
    e = HEAD**-0.5 * LOG2E
    tokens = q_ref.shape[0]
    k, vt = k_ref[:, here], v_ref[:, here].T
    vt = jnp.concatenate([vt, jnp.ones((16, tokens), BF)], axis=0)
    for at in range(0, tokens, QB):
        parts = _scores(k[: at + QB], q_ref[at : at + QB, here], at)
        top = functools.reduce(jnp.maximum, [s.max(axis=0, keepdims=True) for s in parts])
        p = jnp.concatenate([jnp.exp2((s - top) * e).astype(BF) for s in parts], axis=0)
        mix = _dot(vt[:, : at + QB], p, 1, 0)
        total = mix[HEAD : HEAD + 1]
        o_ref[at : at + QB, here] = (mix[:HEAD] * (1 / total)).T.astype(BF)
        lse_ref[pl.ds(h, 1), at : at + QB] = top * e + jnp.log(total) * LOG2E


LANES = [axes[::-1] for axes in (X, Y, Z)]


def _front_kernel(items, *refs):
    x, starts, places, shards, q, k, v, o, h, cos, sin, lse, whole, kept, a, wide, sems, local, keep = refs
    g = _Gather(items, shards, (*wide, *whole), sems, local)
    tokens, d = x.shape
    _greet()
    first, later = [[i for i in range(len(items)) if (items[i][0] < 3) == now] for now in (True, False)]

    def each(f, some, n):
        for i in some:
            f(i, n)

    each(g.start, first, 0)
    each(g.start, later, 0)

    def norm(b):
        rows = pl.ds(b * HEAD, HEAD)
        a[rows, :] = _normed(x[rows, :])

    def tables(b):
        rows, start = pl.ds(b * HEAD, HEAD), pl.ds(b, 1)
        c, s = starts[0, start, :], starts[1, start, :]
        cos[rows, :] = c * places[0] - s * places[1]
        sin[rows, :] = c * places[1] + s * places[0]

    each(g.relay, first, 0)
    each(g.relay, later, 0)
    each(g.finish, first, 0)
    _loop(0, tokens // HEAD, norm)
    each(g.relay, first, 1)
    each(g.finish, later, 0)
    each(g.finish, first, 1)
    _loop(0, tokens // HEAD, tables)
    each(g.relay, later, 1)
    each(g.relay, first, 2)
    each(g.finish, later, 1)
    each(g.finish, first, 2)

    copies = []

    def squared(n):
        copies.append(pltpu.make_async_copy(wide[n], kept[n], keep.at[n]))
        copies[-1].start()
        return wide[n].reshape(x.shape)

    def project(n, out):
        g.arrive(first[n])
        w = squared(n)

        def cols(n):
            t = jnp.dot(a[...], w[:, _cols(n, QB)], preferred_element_type=F32).astype(BF)
            for j in range(QB // HEAD):
                part = t[:, j * HEAD : (j + 1) * HEAD]
                if out is not v:
                    part = _turn(part.astype(F32), cos[...], sin[...]).astype(BF)
                out[:, _cols(n * (QB // HEAD) + j, HEAD)] = part

        _loop(0, d // QB, cols)

    def heads(n):
        _loop(n, n + 2, lambda h: _attend(h, q, k, v, o, lse))

    project(0, q)
    each(g.relay, later, 2)
    project(1, k)
    project(2, v)
    halves = later[:2]
    for n in range(0, d // HEAD, 2):
        heads(n)
        if n == 4:
            each(g.finish, halves, 2)
    each(g.finish, later[2:], 2)
    for i in halves:
        g.arrive(i)
    w = squared(3)

    def add(n):
        here = _cols(n, QB)
        h[:, here] = (x[:, here].astype(F32) + jnp.dot(o[...], w[:, here], preferred_element_type=F32).astype(BF).astype(F32)).astype(BF)

    _loop(0, d // QB, add)
    for i in later[2:]:
        g.arrive(i)
    for c in copies:
        c.wait()
    g.end()


def _call(kernel, number, scratch, ins, out_shape, in_specs, out_specs):
    return pl.pallas_call(
        kernel,
        out_shape=out_shape,
        in_specs=in_specs,
        out_specs=out_specs,
        scratch_shapes=scratch,
        compiler_params=pltpu.CompilerParams(collective_id=number, has_side_effects=True, vmem_limit_bytes=VMEM),
    )(*ins)


def front(x, shards):
    many, near = len(shards), 4
    spread = [jax.ShapeDtypeStruct(_cut((s.shape[0] * 128, s.shape[1])), BF) for s in shards]
    table = jax.ShapeDtypeStruct((x.shape[0], HEAD), F32)
    lse = jax.ShapeDtypeStruct((x.shape[1] // HEAD, x.shape[0]), F32)
    half = HEAD // 2
    rates = np.tile(THETA ** (-np.arange(half) / half), 2)
    sign = np.repeat([-1, 1], half)

    def turns(places):
        angle = places[:, None] * rates
        return np.stack([np.cos(angle), np.sin(angle) * sign]).astype(np.float32)

    whole = [(i, 0, s.shape[1]) for i, s in enumerate(shards)]
    half = shards[3].shape[1] // 2
    axes = *LANES, *LANES
    items = [(*w, a) for w, a in zip(whole[:3] + whole[near:], axes)] + [(3, n * half, half, a) for n, a in enumerate(LANES[:2])]
    items = sorted(items)
    dma = pltpu.SemaphoreType.DMA
    *seen, h, cos, sin, lse, late, early = _call(
        functools.partial(_front_kernel, items), 0,
        [pltpu.VMEM(x.shape, BF), [pltpu.VMEM(s.shape, BF) for s in spread[:near]], dma((len(items), 4, 2, 6)), dma((len(items),)), dma((near,))],
        (x, turns(np.arange(0, x.shape[0], HEAD)), turns(np.arange(HEAD)), shards), (*_like(x) * 5, table, table, lse, spread[near:], spread[:near]),
        (INSIDE, INSIDE, INSIDE, [INSIDE] * many), (*[INSIDE] * 8, [OUTSIDE] * (many - near), [OUTSIDE] * near))
    return seen, h, cos, sin, lse, [w.reshape(-1, w.shape[-1]) for w in (*early, *late)]


def _attend_back(h, q_ref, k_ref, v_ref, do_ref, lse_ref, delta_ref, dk_s, dv_s, cos, sin):
    here = _cols(h, HEAD)
    scale = HEAD**-0.5
    tokens = q_ref.shape[0]
    k, v = k_ref[:, here], v_ref[:, here]
    kt = k.T
    for at in reversed(range(0, tokens, QB)):
        n = at + QB
        rows = slice(at, n)
        q, do = q_ref[rows, here], do_ref[rows, here]
        lse, delta = lse_ref[pl.ds(h, 1), rows], delta_ref[pl.ds(h, 1), rows]
        dp = _dot(v[:n], do, 1, 1)
        p = jnp.concatenate([jnp.exp2(s * (scale * LOG2E) - lse) for s in _scores(k[:n], q, at)], axis=0)
        ds = (p * (dp - delta)).astype(BF)
        by_v, by_k = _dot(p.astype(BF), do, 1, 0), _dot(ds, q, 1, 0)
        if n == tokens:
            dv_s[...] = by_v
            dk_s[...] = by_k
        else:
            dv_s[:n] += by_v
            dk_s[:n] += by_k
        dq = (_dot(kt[:, :n], ds, 1, 0) * scale).T.astype(BF)
        q_ref[rows, here] = _turn(dq.astype(F32), cos[rows], -sin[rows]).astype(BF)
    dk = (dk_s[...] * scale).astype(BF)
    k_ref[:, here] = _turn(dk.astype(F32), cos[...], -sin[...]).astype(BF)
    v_ref[:, here] = dv_s[...].astype(BF)


def _norm_back(h, by_b):
    r = lax.rsqrt(jnp.mean(h * h, -1, keepdims=True) + EPS)
    return r * by_b - h * (r * r * r * jnp.mean(h * by_b, -1, keepdims=True))


def _plus(h, by_h):
    return (h.astype(F32) + by_h.astype(BF).astype(F32)).astype(BF)


def _normed(h):
    h = h.astype(F32)
    return (h * lax.rsqrt(jnp.mean(h * h, -1, keepdims=True) + EPS)).astype(BF)


def _middle_kernel(blocks, *refs):
    h, dy, gate_cols, up_cols, down_rows, gate_rows, up_rows, dh, by_gate, by_up, by_down, b, bt, d_gate, d_up, db = refs
    step = pl.program_id(0)
    tokens, width = h.shape[0], by_gate.shape[1]

    @pl.when(step == 0)
    def _():
        def norm(n):
            rows = pl.ds(pl.multiple_of(n * HEAD, HEAD), HEAD)
            b[rows, :] = _normed(h[rows, :])
            bt[:, rows] = b[rows, :].T

        _loop(0, tokens // HEAD, norm)

    @pl.when(step < blocks)
    def _():
        here = _cols(step, width)
        acts = []
        for at in range(0, tokens, ROWS):
            rows = slice(at, at + ROWS)
            gate, up = _dot(b[rows, :], gate_cols[...], 1, 0), _dot(b[rows, :], up_cols[...], 1, 0)
            by_act = _dot(dy[rows, :], down_rows[...], 1, 1).astype(BF).astype(F32)
            share = lax.logistic(gate)
            silu = gate * share
            acts.append((silu * up).astype(BF))
            d_up[rows, here] = (by_act * silu).astype(BF)
            d_gate[rows, here] = (by_act * up * (share + silu * (1 - share))).astype(BF)
        by_down[...] = _dot(jnp.concatenate([a.T for a in acts], axis=1), dy[...], 1, 0).astype(BF)
        by_gate[...] = _dot(bt[...], d_gate[:, here], 1, 0).astype(BF)
        by_up[...] = _dot(bt[...], d_up[:, here], 1, 0).astype(BF)

    @pl.when(step >= blocks)
    def _():
        db[:, _cols(step - blocks, QB)] = _dot(d_gate[...], gate_rows[...], 1, 1) + _dot(d_up[...], up_rows[...], 1, 1)

    @pl.when(step == pl.num_programs(0) - 1)
    def _():
        def norm(n):
            rows = pl.ds(pl.multiple_of(n * HEAD, HEAD), HEAD)
            dh[rows, :] = _plus(dy[rows, :], _norm_back(h[rows, :].astype(F32), db[rows, :]))

        _loop(0, tokens // HEAD, norm)


ROWS, WIDTH = 512, 256


def middle(h, dy, w_gate, w_up, w_down):
    (tokens, d), ff = h.shape, w_gate.shape[1]
    blocks, more = ff // WIDTH, d // QB
    fixed = pl.BlockSpec((tokens, d), lambda s: (0, 0))
    cols = pl.BlockSpec((d, WIDTH), lambda s: (0, jnp.minimum(s, blocks - 1)))
    rows = pl.BlockSpec((WIDTH, d), lambda s: (jnp.minimum(s, blocks - 1), 0))
    across = pl.BlockSpec((QB, ff), lambda s: (jnp.maximum(s - blocks, 0), 0))
    square, wide = pltpu.VMEM(h.shape, BF), pltpu.VMEM((tokens, ff), BF)
    return pl.pallas_call(
        functools.partial(_middle_kernel, blocks),
        grid=(blocks + more,),
        out_shape=_like(h, w_gate, w_up, w_down),
        in_specs=[fixed, fixed, cols, cols, rows, across, across],
        out_specs=[fixed, cols, cols, rows],
        scratch_shapes=[square, square, wide, wide, pltpu.VMEM(h.shape, F32)],
        compiler_params=pltpu.CompilerParams(dimension_semantics=("arbitrary",), vmem_limit_bytes=VMEM),
    )(h, dy, w_gate, w_up, w_down, w_gate, w_up)


def _back_kernel(items, *refs):
    x, cos, sin, dh, lse, far, weights, terms, dx, grads, mine, near, w, at, stage, delta, dk_s, dv_s, load, store, scratch = refs
    s = _Scatter(items, (*terms, *grads), mine, *scratch)
    q, k, v, o = near
    tokens, d = x.shape
    _greet()
    early, late = [i for i in range(len(items)) if items[i][0] < 3 or items[i][0] == 6], range(3, 6)
    s.begin(*early[:3])
    wq, wk, wv, wo = weights
    pairs = [(far[3], o), (wo, w.at[0]), *zip(far, (q, k, v)), (wk, w.at[1]), (wv, w.at[2]), (wq, w.at[0])]
    loads = [pltpu.make_async_copy(src, dst, load.at[n]) for n, (src, dst) in enumerate(pairs)]
    get_o, get_wo, *get_qkv, get_wk, get_wv, get_wq = loads
    for c in loads[:-1]:
        c.start()
    flat = [g.reshape(d, d) for g in grads]
    stores = [pltpu.make_async_copy(src, dst, store.at[n]) for n, (src, dst) in enumerate(zip((o, stage, o, stage), flat))]
    put_q, put_k, put_v, put_o = stores

    def transposed():
        def body(n):
            at[:, _cols(n, HEAD)] = _normed(x[pl.ds(n * HEAD, HEAD), :]).T

        _loop(0, tokens // HEAD, body)
        get_o.wait()

    def by_wo(n):
        stage[pl.ds(n * QB, QB), :] = _dot(o[:, _cols(n, QB)].T, dh[...], 1, 0).astype(BF)

    def wo_done():
        put_o.start()
        get_wo.wait()

    def by_o(n):
        do = _dot(dh[...], w[0, pl.ds(n * QB, QB), :], 1, 1).astype(BF)
        for j in range(QB // HEAD):
            h = n * (QB // HEAD) + j
            here, part = _cols(h, HEAD), do[:, j * HEAD : (j + 1) * HEAD]
            product = part.astype(F32) * o[:, here].astype(F32)
            delta[pl.ds(h, 1), :] = product.T.sum(axis=0, keepdims=True)
            o[:, here] = part

    def o_begun():
        put_o.wait()
        s.begin(*early[3:])

    def o_done():
        for c in get_qkv:
            c.wait()
        get_wq.start()

    def head(h):
        _attend_back(h, q, k, v, o, lse, delta, dk_s, dv_s, cos, sin)

    def by_weight(i, into, put):
        def body(n):
            here = _cols(n, QB)
            into[:, here] = jnp.dot(at[...], near[i][:, here], preferred_element_type=F32).astype(BF)

        _loop(0, d // QB, body)
        put.start()

    def weight_done(i, put):
        put.wait()
        s.begin(3 + i)

    def by_x(b):
        rows = pl.ds(b * QB, QB)
        da = _dot(q[rows, :], w[0], 1, 1) + _dot(k[rows, :], w[1], 1, 1) + _dot(v[rows, :], w[2], 1, 1)
        at[rows, :] = _plus(dh[rows, :], _norm_back(x[rows, :].astype(F32), da))

    big, small = early[:3], early[3:]

    def merge(some, *ds):
        for d in ds:
            s.merge(d, *some)

    def relay(some, k):
        for i in some:
            s.relay(i, k)

    def finish(some, k):
        for i in some:
            s.finish(i, k)

    q_item, k_item, v_item = ([i] for i in late)
    transposed()
    _loop(0, 2, by_wo)
    merge(big, 2)
    _loop(2, d // QB, by_wo)
    wo_done()
    merge(big, UP)
    _loop(0, 2, by_o)
    o_begun()
    merge(big, DOWN)
    _loop(2, d // QB, by_o)
    o_done()
    merge(big, 0)
    _loop(0, 2, head)
    relay(big, 1)
    merge(small, 2, UP)
    _loop(2, 4, head)
    merge(small, DOWN, 0)
    _loop(4, 6, head)
    relay(small, 1)
    _loop(6, d // HEAD, head)
    by_weight(0, o, put_q)
    by_weight(1, stage, put_k)
    weight_done(0, put_q)
    by_weight(2, o, put_v)
    weight_done(1, put_k)
    merge(q_item, *ORDER)
    finish(big, 1)
    weight_done(2, put_v)
    merge(k_item, *ORDER)
    finish(small, 1)
    merge(v_item, *ORDER)
    for c in (get_wk, get_wv, get_wq):
        c.wait()
    by_x(0)
    relay(late, 1)
    relay(big, 2)
    by_x(1)
    relay(small, 2)
    finish(late, 1)
    by_x(2)
    finish(big, 2)
    relay(late, 2)
    by_x(3)
    put_x = pltpu.make_async_copy(at, dx, load.at[0])
    put_x.start()
    finish(small, 2)
    finish(late, 2)
    finish(big, 3)
    finish(small, 3)
    finish(late, 3)
    put_x.wait()
    s.end()


def back(x, cos, sin, dh, lse, seen, weights, terms):
    d = x.shape[1]
    items = [(0, 0, 8, 0, 3 * d, X), (1, 0, 8, 0, 3 * d, Y), (2, 0, 24, 0, d, Z), *((3 + n, 0, 8, 0, d, axes) for n, axes in enumerate((X, Y, Z))),
             *((6, 0, 8, n * d // 2, d // 2, axes) for n, axes in enumerate((X, Y)))]
    square, column, dma = pltpu.VMEM(x.shape, BF), pltpu.VMEM((x.shape[0], HEAD), F32), pltpu.SemaphoreType.DMA
    blocks = [jax.ShapeDtypeStruct((item[2], item[4]), BF) for item in items]
    dx, _, (gate, up, down, *four) = _call(
        functools.partial(_back_kernel, items), 1,
        [[square] * 4, pltpu.VMEM((3, *x.shape), BF), square, square, pltpu.VMEM(lse.shape, F32), column, column, dma((8,)), dma((4,)), _scatter_scratch(items)],
        (x, cos, sin, dh, lse, seen, weights, [t.reshape(_cut(t.shape)) for t in terms]),
        (*_like(x), [jax.ShapeDtypeStruct(_cut(x.shape), BF)] * 4, blocks),
        (INSIDE, INSIDE, INSIDE, INSIDE, INSIDE, [OUTSIDE] * 4, [OUTSIDE] * 4, [OUTSIDE] * 3), (OUTSIDE, [OUTSIDE] * 4, [INSIDE] * len(items)))
    return dx, (*four, gate, up, down)


def _last_kernel(dx_in, q, k, v, left, right, gate, up, down, dx, *outs):
    dx[0] = dx_in[...]
    for out, ref in zip((*outs[:3], *outs[4:]), (q, k, v, gate, up, down)):
        out[0] = ref[...]
    half = left.shape[1]
    outs[3][0, :, :half] = left[...]
    outs[3][0, :, half:] = right[...]


def last(dx, blocks, shapes):
    return pl.pallas_call(_last_kernel, out_shape=[jax.ShapeDtypeStruct(s, BF) for s in shapes], in_specs=[INSIDE] * (1 + len(blocks)),
                          out_specs=[INSIDE] * len(shapes))(dx, *blocks)


def solution(mesh):
    def step(x, dy, *weights):
        shapes = [a.shape for a in (x, *weights)]
        x, dy = x[0], dy[0]
        seen, h, cos, sin, lse, whole = front(x, [w[0] for w in weights])
        dh, *terms = middle(h, dy, *whole[4:])
        dx, blocks = back(x, cos, sin, dh, lse, seen, whole[:4], terms)
        return tuple(last(dx, blocks, shapes))

    states, cut = P(("rep", "dp"), None, None), P(None, "dp", None)
    return jax.shard_map(
        step,
        mesh=mesh,
        in_specs=(states, states) + (cut,) * 7,
        out_specs=(states,) + (P("rep", "dp", None),) * 7,
        check_vma=False,
    )
```

```python
import functools
import math

import jax
import jax.numpy as jnp
import numpy as np
from jax import lax
from jax.experimental import pallas as pl
from jax.experimental.pallas import tpu as pltpu
from jax.sharding import PartitionSpec as P

BF, F32 = jnp.bfloat16, jnp.float32
HIDDEN = -2e30
LOG2E = 1.4426950408889634
VMEM = 63 * 2**20
EPS = 1e-6
HEAD = 128
THETA = 10000
NAMES = ("wq", "wk", "wv", "wo", "w_gate", "w_up", "w_down")
QB = 256
ALL = slice(None)
INSIDE, OUTSIDE = pl.BlockSpec(memory_space=pltpu.VMEM), pl.BlockSpec(memory_space=pl.ANY)


def _loop(first, last, body):
    lax.fori_loop(first, last, lambda b, _: body(b), None)


def _like(*arrays):
    return [jax.ShapeDtypeStruct(a.shape, BF) for a in arrays]


STRIDE = (32, 8, 2)
X, Y, Z = (0, 1, 2), (1, 2, 0), (2, 0, 1)
RING, UP, DOWN = 4, 1, 3
ORDER = 2, UP, DOWN, 0


def _place():
    me = lax.axis_index("dp")
    return me, [me // s % RING for s in STRIDE], me % 2


def _peer(me, at, axis, by):
    return me + ((at[axis] + by) % RING - at[axis]) * STRIDE[axis]


def _send(src, dst, send, recv, to):
    c = pltpu.make_async_remote_copy(src_ref=src, dst_ref=dst, send_sem=send, recv_sem=recv, device_id={"dp": to}, device_id_type=pl.DeviceIdType.MESH)
    c.start()
    return c


def _greet():
    me, at, core = _place()
    barrier = pltpu.get_barrier_semaphore()
    peers = [me + 1 - 2 * core] + [_peer(me, at, axis, by) for axis in range(3) for by in (UP, 2, DOWN)]
    for p in peers:
        pl.semaphore_signal(barrier, inc=1, device_id={"dp": p}, device_id_type=pl.DeviceIdType.MESH)
    pl.semaphore_wait(barrier, len(peers))


def _spot(ref, depth, b):
    return (lambda: ref, lambda: ref.at[b], lambda: ref.at[b // RING, b % RING])[depth]()


def _add(terms, dst, depth, spot=None):
    def body(b):
        values = [(spot or _spot)(t, depth, b)[...].astype(F32) for t in terms]
        _spot(dst, depth, b)[...] = functools.reduce(jnp.add, values).astype(BF)

    _loop(0, math.prod(dst.shape[:depth]), body)


class _Scatter:
    def __init__(self, items, ins, outs, sems, loads, *bufs):
        self.items, self.ins, self.outs, self.sems, self.loads = items, ins, outs, sems, loads
        per = len(bufs) // len(items)
        self.bufs = [bufs[per * i : per * (i + 1)] for i in range(len(items))]
        self.me, self.at, self.core = _place()
        self.sent, self.flights, self.own = [], {}, {}

    def source(self, i, d, c):
        ref, row, rows, first, cols, axes = self.items[i]
        index = [ALL] * 3
        index[axes[0]] = (self.at[axes[0]] + d) % RING
        return self.ins[ref].at[(*index, c, pl.ds(row, rows), pl.ds(first, cols))]

    def pair(self, i, k, slot):
        return self.sems.at[i, k, 0, slot], self.sems.at[i, k, 1, slot]

    def begin(self, *some):
        for d in ORDER:
            for i in some:
                c = _send(self.source(i, d, 1 - self.core), self.bufs[i][0].at[d], *self.pair(i, 0, d), self.me + 1 - 2 * self.core)
                self.flights[i, 0, d] = c
                self.sent.append(c)
                if d == 2 or _little(_kind(self.items[i])):
                    self.fetch(i, d)

    def fetch(self, i, d):
        room = self.bufs[i][-1].at[d] if _little(_kind(self.items[i])) else self.bufs[i][4]
        self.own[i, d] = room, pltpu.make_async_copy(self.source(i, d, self.core), room, self.loads.at[i, d])
        self.own[i, d][1].start()

    def merge(self, d, *some):
        for i in some:
            acc = self.bufs[i][0].at[d]
            self.flights[i, 0, d].wait_recv()
            room, load = self.own[i, d]
            load.wait()
            _add([acc, room], acc, 2)
            if d == 2:
                self.first_out(i, 1)
            if d == DOWN:
                self.second_out(i, 1)
            if d and not _little(_kind(self.items[i])):
                self.fetch(i, ORDER[ORDER.index(d) + 1])

    def half(self, i, k, ref, h):
        return ref.at[pl.ds(2 * h, 2)]

    def post(self, i, k, slot, src, dst, by):
        c = _send(src, dst, *self.pair(i, k, slot), _peer(self.me, self.at, self.items[i][5][k - 1], by))
        self.flights[i, k, slot] = c
        self.sent.append(c)

    def phase(self, i, k):
        return self.bufs[i][4 * k - 4 : 4 * k]

    def first_out(self, i, k):
        acc, early, low, high = self.phase(i, k)
        if k == 3:
            self.post(i, k, 0, acc.at[2], early, 2)
            self.post(i, k, 2, acc.at[UP], low, UP)
            self.post(i, k, 3, acc.at[DOWN], high, DOWN)
            return
        for slot, by in enumerate((UP, DOWN)):
            self.post(i, k, slot, self.half(i, k, acc.at[2], slot), early.at[slot], by)

    def second_out(self, i, k):
        acc, early, low, high = self.phase(i, k)
        for slot, by, h, land in ((2, UP, 1, low), (3, DOWN, 0, high)):
            self.post(i, k, slot, self.half(i, k, acc.at[by], h), self.half(i, k, land, h), by)

    def relay(self, i, k):
        acc, early, low, high = self.phase(i, k)
        for slot, d, land in ((0, UP, low), (1, DOWN, high)):
            self.flights[i, k, slot].wait_recv()
            part = self.half(i, k, acc.at[d], slot)
            _add([part, early.at[slot]], part, 3 - k)
            self.post(i, k, 4 + slot, part, self.half(i, k, land, slot), d)

    def finish(self, i, k):
        acc, early, low, high = self.phase(i, k)
        for slot in (0, 2, 3) if k == 3 else (2, 3, 4, 5):
            self.flights[i, k, slot].wait_recv()
        *_, (_, second, third) = self.items[i]

        def shifted(ref, depth, b):
            s, t = (self.at[second] + b // RING) % RING, (self.at[third] + b % RING) % RING
            return ref.at[(s, t) if second < third else (t, s)]

        terms = [acc.at[0], low, high, early]
        _add(terms if k == 3 else terms[:3], self.outs[i] if k == 3 else self.bufs[i][4 * k], 3 - k, shifted if k == 1 else None)
        if k < 3:
            self.first_out(i, k + 1)
        if k < 2:
            self.second_out(i, k + 1)

    def end(self):
        for c in self.sent:
            c.wait_send()


def _little(kind):
    return math.prod(kind) <= 8 * 1024


def _kind(item):
    return item[2], item[4]


def _scatter_scratch(items):
    def room(*shape):
        return pltpu.VMEM(shape, BF)

    scratch = []
    for kind in map(_kind, items):
        for ring in ((RING, RING), (RING,)):
            scratch += [room(RING, *ring, *kind), room(2, 2, *ring[1:], *kind), room(*ring, *kind), room(*ring, *kind)]
        scratch += [room(RING, *kind), room(*kind), room(*kind), room(*kind), room(*((RING,) * 3 if _little(kind) else ()), *kind)]
    return [pltpu.SemaphoreType.DMA((len(items), 4, 2, 6)), pltpu.SemaphoreType.DMA((len(items), RING)), *scratch]


def _cut(shape):
    return RING, RING, RING, 2, shape[0] // 128, shape[1]


class _Gather:
    def __init__(self, items, ins, outs, sems, local):
        self.items, self.ins, self.outs, self.sems, self.local = items, ins, outs, sems, local
        self.me, self.at, self.core = _place()
        self.sent, self.flights, self.mine = [], {}, {}

    def region(self, i, full, by=None, part=None):
        index = [ALL if a in full else self.at[a] for a in range(3)]
        if by is not None:
            axis, d = by
            index[axis] = (self.at[axis] + d) % RING
        ref = self.items[i][0]
        if part is not None and full:
            index[full[0]] = pl.ds(2 * part, 2)
            part = None
        return self.outs[ref].at[(*index, self.core, ALL, self.columns(i, part))]

    def columns(self, i, part):
        _, first, width, _ = self.items[i]
        half = width // 2
        return pl.ds(first, width) if part is None else pl.ds(first + part * half, half)

    def own(self, i, part):
        return self.ins[self.items[i][0]].at[:, self.columns(i, part)]

    def post(self, i, k, slot, src, dst, to):
        c = _send(src, dst, self.sems.at[i, k, 0, slot], self.sems.at[i, k, 1, slot], to)
        self.flights[i, k, slot] = c
        self.sent.append(c)

    def short(self, i, k):
        return k == 0 or k == 1 and self.items[i][0] < 3

    def along(self, i, k):
        *_, axes = self.items[i]
        axis = axes[k]
        return axis, axes[:k], *[_peer(self.me, self.at, axis, by) for by in (UP, DOWN)]

    def start(self, i, k):
        axis, full, up, down = self.along(i, k)
        plan = (0, 0, up), (1, 1, down), (2, 1, up), (3, 0, down)
        if self.short(i, k):
            plan = (2, None, up), (3, None, down), (4, None, _peer(self.me, self.at, axis, 2))
        for slot, part, to in plan:
            there = self.region(i, full, None, part)
            self.post(i, k, slot, there if k else self.own(i, part), there, to)
        if k == 0:
            self.mine[i] = pltpu.make_async_copy(self.own(i, None), self.region(i, ()), self.local.at[i])
            self.mine[i].start()
        if k == 2:
            self.across(i, 0, 0)

    def across(self, i, slot, by):
        axis, full, _, _ = self.along(i, 2)
        piece = self.region(i, full, (axis, by))
        self.post(i, 3, slot, piece, piece, self.me + 1 - 2 * self.core)

    def relay(self, i, k):
        axis, full, up, down = self.along(i, k)
        if self.short(i, k):
            return
        for slot, by, to in ((0, DOWN, up), (1, UP, down)):
            self.flights[i, k, slot].wait_recv()
            piece = self.region(i, full, (axis, by), slot)
            self.post(i, k, 4 + slot, piece, piece, to)

    def finish(self, i, k):
        for slot in (2, 3):
            self.flights[i, k, slot].wait_recv()
        if k == 0:
            self.mine[i].wait()
        if k == 2:
            self.across(i, 1, UP)
            self.across(i, 2, DOWN)
        for slot in (4,) if self.short(i, k) else (4, 5):
            self.flights[i, k, slot].wait_recv()
        if k == 2:
            self.across(i, 3, 2)
        else:
            self.start(i, k + 1)

    def arrive(self, i):
        for slot in range(4):
            self.flights[i, 3, slot].wait_recv()

    def end(self):
        for c in self.sent:
            c.wait_send()


def _dot(a, b, ca, cb):
    return lax.dot_general(a, b, (((ca,), (cb,)), ((), ())), preferred_element_type=F32)


def _cols(n, width):
    return pl.ds(pl.multiple_of(n * width, width), width)


def _turn(t, cos, sin):
    return t * cos + pltpu.roll(t, HEAD // 2, 1) * sin


def _scores(k, q, first):
    n = k.shape[0] - first
    low = lax.broadcasted_iota(jnp.int32, (n, q.shape[0]), 0) <= lax.broadcasted_iota(jnp.int32, (n, q.shape[0]), 1)
    diagonal = jnp.where(low, _dot(k[first:], q, 1, 1), HIDDEN)
    return ([_dot(k[:first], q, 1, 1)] if first else []) + [diagonal]


def _attend(h, q_ref, k_ref, v_ref, o_ref, lse_ref):
    here = _cols(h, HEAD)
    e = HEAD**-0.5 * LOG2E
    tokens = q_ref.shape[0]
    k, vt = k_ref[:, here], v_ref[:, here].T
    vt = jnp.concatenate([vt, jnp.ones((16, tokens), BF)], axis=0)
    for at in range(0, tokens, QB):
        parts = _scores(k[: at + QB], q_ref[at : at + QB, here], at)
        top = functools.reduce(jnp.maximum, [s.max(axis=0, keepdims=True) for s in parts])
        p = jnp.concatenate([jnp.exp2((s - top) * e).astype(BF) for s in parts], axis=0)
        mix = _dot(vt[:, : at + QB], p, 1, 0)
        total = mix[HEAD : HEAD + 1]
        o_ref[at : at + QB, here] = (mix[:HEAD] * (1 / total)).T.astype(BF)
        lse_ref[pl.ds(h, 1), at : at + QB] = top * e + jnp.log(total) * LOG2E


LANES = [axes[::-1] for axes in (X, Y, Z)]


def _front_kernel(items, *refs):
    x, starts, places, shards, q, k, v, o, h, cos, sin, lse, whole, kept, a, wide, sems, local, keep = refs
    g = _Gather(items, shards, (*wide, *whole), sems, local)
    tokens, d = x.shape
    _greet()
    first, later = [[i for i in range(len(items)) if (items[i][0] < 3) == now] for now in (True, False)]

    def each(f, some, n):
        for i in some:
            f(i, n)

    each(g.start, first, 0)
    each(g.start, later, 0)

    def norm(b):
        rows = pl.ds(b * HEAD, HEAD)
        a[rows, :] = _normed(x[rows, :])

    def tables(b):
        rows, start = pl.ds(b * HEAD, HEAD), pl.ds(b, 1)
        c, s = starts[0, start, :], starts[1, start, :]
        cos[rows, :] = c * places[0] - s * places[1]
        sin[rows, :] = c * places[1] + s * places[0]

    each(g.relay, first, 0)
    each(g.relay, later, 0)
    each(g.finish, first, 0)
    _loop(0, tokens // HEAD, norm)
    each(g.relay, first, 1)
    each(g.finish, later, 0)
    each(g.finish, first, 1)
    _loop(0, tokens // HEAD, tables)
    each(g.relay, later, 1)
    each(g.relay, first, 2)
    each(g.finish, later, 1)
    each(g.finish, first, 2)

    copies = []

    def squared(n):
        copies.append(pltpu.make_async_copy(wide[n], kept[n], keep.at[n]))
        copies[-1].start()
        return wide[n].reshape(x.shape)

    def project(n, out):
        g.arrive(first[n])
        w = squared(n)

        def cols(n):
            t = jnp.dot(a[...], w[:, _cols(n, QB)], preferred_element_type=F32).astype(BF)
            for j in range(QB // HEAD):
                part = t[:, j * HEAD : (j + 1) * HEAD]
                if out is not v:
                    part = _turn(part.astype(F32), cos[...], sin[...]).astype(BF)
                out[:, _cols(n * (QB // HEAD) + j, HEAD)] = part

        _loop(0, d // QB, cols)

    def head(n):
        _attend(n, q, k, v, o, lse)

    project(0, q)
    each(g.relay, later, 2)
    project(1, k)
    project(2, v)
    halves = later[:2]
    _loop(0, d // HEAD - 2, head)
    each(g.finish, halves, 2)
    _loop(d // HEAD - 2, d // HEAD, head)
    each(g.finish, later[2:], 2)
    for i in halves:
        g.arrive(i)
    w = squared(3)

    def add(n):
        here = _cols(n, QB)
        h[:, here] = (x[:, here].astype(F32) + jnp.dot(o[...], w[:, here], preferred_element_type=F32).astype(BF).astype(F32)).astype(BF)

    _loop(0, d // QB, add)
    for i in later[2:]:
        g.arrive(i)
    for c in copies:
        c.wait()
    g.end()


def _call(kernel, number, scratch, ins, out_shape, in_specs, out_specs):
    return pl.pallas_call(
        kernel,
        out_shape=out_shape,
        in_specs=in_specs,
        out_specs=out_specs,
        scratch_shapes=scratch,
        compiler_params=pltpu.CompilerParams(collective_id=number, has_side_effects=True, vmem_limit_bytes=VMEM),
    )(*ins)


def front(x, shards):
    many, near = len(shards), 4
    spread = [jax.ShapeDtypeStruct(_cut((s.shape[0] * 128, s.shape[1])), BF) for s in shards]
    table = jax.ShapeDtypeStruct((x.shape[0], HEAD), F32)
    lse = jax.ShapeDtypeStruct((x.shape[1] // HEAD, x.shape[0]), F32)
    half = HEAD // 2
    rates = np.tile(THETA ** (-np.arange(half) / half), 2)
    sign = np.repeat([-1, 1], half)

    def turns(places):
        angle = places[:, None] * rates
        return np.stack([np.cos(angle), np.sin(angle) * sign]).astype(np.float32)

    whole = [(i, 0, s.shape[1]) for i, s in enumerate(shards)]
    half = shards[3].shape[1] // 2
    axes = *LANES, *LANES
    items = [(*w, a) for w, a in zip(whole[:3] + whole[near:], axes)] + [(3, n * half, half, a) for n, a in enumerate(LANES[:2])]
    items = sorted(items)
    dma = pltpu.SemaphoreType.DMA
    *seen, h, cos, sin, lse, late, early = _call(
        functools.partial(_front_kernel, items), 0,
        [pltpu.VMEM(x.shape, BF), [pltpu.VMEM(s.shape, BF) for s in spread[:near]], dma((len(items), 4, 2, 6)), dma((len(items),)), dma((near,))],
        (x, turns(np.arange(0, x.shape[0], HEAD)), turns(np.arange(HEAD)), shards), (*_like(x) * 5, table, table, lse, spread[near:], spread[:near]),
        (INSIDE, INSIDE, INSIDE, [INSIDE] * many), (*[INSIDE] * 8, [OUTSIDE] * (many - near), [OUTSIDE] * near))
    return seen, h, cos, sin, lse, [w.reshape(-1, w.shape[-1]) for w in (*early, *late)]


def _attend_back(h, q_ref, k_ref, v_ref, do_ref, lse_ref, delta_ref, dk_s, dv_s, cos, sin):
    here = _cols(h, HEAD)
    scale = HEAD**-0.5
    tokens = q_ref.shape[0]
    k, v = k_ref[:, here], v_ref[:, here]
    kt = k.T
    for at in reversed(range(0, tokens, QB)):
        n = at + QB
        rows = slice(at, n)
        q, do = q_ref[rows, here], do_ref[rows, here]
        lse, delta = lse_ref[pl.ds(h, 1), rows], delta_ref[pl.ds(h, 1), rows]
        dp = _dot(v[:n], do, 1, 1)
        p = jnp.concatenate([jnp.exp2(s * (scale * LOG2E) - lse) for s in _scores(k[:n], q, at)], axis=0)
        ds = (p * (dp - delta)).astype(BF)
        by_v, by_k = _dot(p.astype(BF), do, 1, 0), _dot(ds, q, 1, 0)
        if n == tokens:
            dv_s[...] = by_v
            dk_s[...] = by_k
        else:
            dv_s[:n] += by_v
            dk_s[:n] += by_k
        dq = (_dot(kt[:, :n], ds, 1, 0) * scale).T.astype(BF)
        q_ref[rows, here] = _turn(dq.astype(F32), cos[rows], -sin[rows]).astype(BF)
    dk = (dk_s[...] * scale).astype(BF)
    k_ref[:, here] = _turn(dk.astype(F32), cos[...], -sin[...]).astype(BF)
    v_ref[:, here] = dv_s[...].astype(BF)


def _norm_back(h, by_b):
    r = lax.rsqrt(jnp.mean(h * h, -1, keepdims=True) + EPS)
    return r * by_b - h * (r * r * r * jnp.mean(h * by_b, -1, keepdims=True))


def _plus(h, by_h):
    return (h.astype(F32) + by_h.astype(BF).astype(F32)).astype(BF)


def _normed(h):
    h = h.astype(F32)
    return (h * lax.rsqrt(jnp.mean(h * h, -1, keepdims=True) + EPS)).astype(BF)


def _middle_kernel(blocks, *refs):
    h, dy, gate_cols, up_cols, down_rows, gate_rows, up_rows, dh, by_gate, by_up, by_down, b, bt, d_gate, d_up, db = refs
    step = pl.program_id(0)
    tokens, width = h.shape[0], by_gate.shape[1]

    @pl.when(step == 0)
    def _():
        def norm(n):
            rows = pl.ds(pl.multiple_of(n * HEAD, HEAD), HEAD)
            b[rows, :] = _normed(h[rows, :])
            bt[:, rows] = b[rows, :].T

        _loop(0, tokens // HEAD, norm)

    @pl.when(step < blocks)
    def _():
        here = _cols(step, width)
        acts = []
        for at in range(0, tokens, ROWS):
            rows = slice(at, at + ROWS)
            gate, up = _dot(b[rows, :], gate_cols[...], 1, 0), _dot(b[rows, :], up_cols[...], 1, 0)
            by_act = _dot(dy[rows, :], down_rows[...], 1, 1).astype(BF).astype(F32)
            share = lax.logistic(gate)
            silu = gate * share
            acts.append((silu * up).astype(BF))
            d_up[rows, here] = (by_act * silu).astype(BF)
            d_gate[rows, here] = (by_act * up * (share + silu * (1 - share))).astype(BF)
        by_down[...] = _dot(jnp.concatenate([a.T for a in acts], axis=1), dy[...], 1, 0).astype(BF)
        by_gate[...] = _dot(bt[...], d_gate[:, here], 1, 0).astype(BF)
        by_up[...] = _dot(bt[...], d_up[:, here], 1, 0).astype(BF)

    @pl.when(step >= blocks)
    def _():
        db[:, _cols(step - blocks, QB)] = _dot(d_gate[...], gate_rows[...], 1, 1) + _dot(d_up[...], up_rows[...], 1, 1)

    @pl.when(step == pl.num_programs(0) - 1)
    def _():
        def norm(n):
            rows = pl.ds(pl.multiple_of(n * HEAD, HEAD), HEAD)
            dh[rows, :] = _plus(dy[rows, :], _norm_back(h[rows, :].astype(F32), db[rows, :]))

        _loop(0, tokens // HEAD, norm)


ROWS, WIDTH = 512, 256


def middle(h, dy, w_gate, w_up, w_down):
    (tokens, d), ff = h.shape, w_gate.shape[1]
    blocks, more = ff // WIDTH, d // QB
    fixed = pl.BlockSpec((tokens, d), lambda s: (0, 0))
    cols = pl.BlockSpec((d, WIDTH), lambda s: (0, jnp.minimum(s, blocks - 1)))
    rows = pl.BlockSpec((WIDTH, d), lambda s: (jnp.minimum(s, blocks - 1), 0))
    across = pl.BlockSpec((QB, ff), lambda s: (jnp.maximum(s - blocks, 0), 0))
    square, wide = pltpu.VMEM(h.shape, BF), pltpu.VMEM((tokens, ff), BF)
    return pl.pallas_call(
        functools.partial(_middle_kernel, blocks),
        grid=(blocks + more,),
        out_shape=_like(h, w_gate, w_up, w_down),
        in_specs=[fixed, fixed, cols, cols, rows, across, across],
        out_specs=[fixed, cols, cols, rows],
        scratch_shapes=[square, square, wide, wide, pltpu.VMEM(h.shape, F32)],
        compiler_params=pltpu.CompilerParams(dimension_semantics=("arbitrary",), vmem_limit_bytes=VMEM),
    )(h, dy, w_gate, w_up, w_down, w_gate, w_up)


def _back_kernel(items, *refs):
    x, cos, sin, dh, lse, far, weights, terms, dx, grads, mine, near, w, at, stage, delta, dk_s, dv_s, load, store, scratch = refs
    s = _Scatter(items, (*terms, *grads), mine, *scratch)
    q, k, v, o = near
    tokens, d = x.shape
    _greet()
    early, late = [i for i in range(len(items)) if items[i][0] < 3 or items[i][0] == 6], range(3, 6)
    s.begin(*early[:3])
    wq, wk, wv, wo = weights
    pairs = [(far[3], o), (wo, w.at[0]), *zip(far, (q, k, v)), (wk, w.at[1]), (wv, w.at[2]), (wq, w.at[0])]
    loads = [pltpu.make_async_copy(src, dst, load.at[n]) for n, (src, dst) in enumerate(pairs)]
    get_o, get_wo, *get_qkv, get_wk, get_wv, get_wq = loads
    for c in loads[:-1]:
        c.start()
    flat = [g.reshape(d, d) for g in grads]
    stores = [pltpu.make_async_copy(src, dst, store.at[n]) for n, (src, dst) in enumerate(zip((o, stage, o, stage), flat))]
    put_q, put_k, put_v, put_o = stores

    def transposed():
        def body(n):
            at[:, _cols(n, HEAD)] = _normed(x[pl.ds(n * HEAD, HEAD), :]).T

        _loop(0, tokens // HEAD, body)
        get_o.wait()

    def by_wo(n):
        stage[pl.ds(n * QB, QB), :] = _dot(o[:, _cols(n, QB)].T, dh[...], 1, 0).astype(BF)

    def wo_done():
        put_o.start()
        get_wo.wait()

    def by_o(n):
        do = _dot(dh[...], w[0, pl.ds(n * QB, QB), :], 1, 1).astype(BF)
        for j in range(QB // HEAD):
            h = n * (QB // HEAD) + j
            here, part = _cols(h, HEAD), do[:, j * HEAD : (j + 1) * HEAD]
            product = part.astype(F32) * o[:, here].astype(F32)
            delta[pl.ds(h, 1), :] = product.T.sum(axis=0, keepdims=True)
            o[:, here] = part

    def o_begun():
        put_o.wait()
        s.begin(*early[3:])

    def o_done():
        for c in get_qkv:
            c.wait()
        get_wq.start()

    def head(h):
        _attend_back(h, q, k, v, o, lse, delta, dk_s, dv_s, cos, sin)

    def by_weight(i, into, put):
        def body(n):
            here = _cols(n, QB)
            into[:, here] = jnp.dot(at[...], near[i][:, here], preferred_element_type=F32).astype(BF)

        _loop(0, d // QB, body)
        put.start()

    def weight_done(i, put):
        put.wait()
        s.begin(3 + i)

    def by_x(b):
        rows = pl.ds(pl.multiple_of(b * QB, QB), QB)
        da = _dot(q[rows, :], w[0], 1, 1) + _dot(k[rows, :], w[1], 1, 1) + _dot(v[rows, :], w[2], 1, 1)
        at[rows, :] = _plus(dh[rows, :], _norm_back(x[rows, :].astype(F32), da))

    big, small = early[:3], early[3:]

    def merge(some, *ds):
        for d in ds:
            s.merge(d, *some)

    def relay(some, k):
        for i in some:
            s.relay(i, k)

    def finish(some, k):
        for i in some:
            s.finish(i, k)

    q_item, k_item, v_item = ([i] for i in late)
    transposed()
    _loop(0, 2, by_wo)
    merge(big, 2)
    _loop(2, d // QB, by_wo)
    wo_done()
    merge(big, UP)
    _loop(0, 2, by_o)
    o_begun()
    merge(big, DOWN)
    _loop(2, d // QB, by_o)
    o_done()
    merge(big, 0)
    _loop(0, 2, head)
    relay(big, 1)
    merge(small, *ORDER)
    _loop(2, 6, head)
    relay(small, 1)
    _loop(6, d // HEAD, head)
    by_weight(0, o, put_q)
    by_weight(1, stage, put_k)
    weight_done(0, put_q)
    by_weight(2, o, put_v)
    weight_done(1, put_k)
    merge(q_item, *ORDER)
    finish(big, 1)
    weight_done(2, put_v)
    merge(k_item, *ORDER)
    finish(small, 1)
    merge(v_item, *ORDER)
    for c in (get_wk, get_wv, get_wq):
        c.wait()
    _loop(0, 2, by_x)
    relay(late, 1)
    relay(big, 2)
    relay(small, 2)
    finish(late, 1)
    _loop(2, tokens // QB, by_x)
    finish(big, 2)
    relay(late, 2)
    put_x = pltpu.make_async_copy(at, dx, load.at[0])
    put_x.start()
    finish(small, 2)
    finish(late, 2)
    finish(big, 3)
    finish(small, 3)
    finish(late, 3)
    put_x.wait()
    s.end()


def back(x, cos, sin, dh, lse, seen, weights, terms):
    d = x.shape[1]
    items = [(0, 0, 8, 0, 3 * d, X), (1, 0, 8, 0, 3 * d, Y), (2, 0, 24, 0, d, Z), *((3 + n, 0, 8, 0, d, axes) for n, axes in enumerate((X, Y, Z))),
             *((6, 0, 8, n * d // 2, d // 2, axes) for n, axes in enumerate((X, Y)))]
    square, column, dma = pltpu.VMEM(x.shape, BF), pltpu.VMEM((x.shape[0], HEAD), F32), pltpu.SemaphoreType.DMA
    blocks = [jax.ShapeDtypeStruct((item[2], item[4]), BF) for item in items]
    dx, _, (gate, up, down, *four) = _call(
        functools.partial(_back_kernel, items), 1,
        [[square] * 4, pltpu.VMEM((3, *x.shape), BF), square, square, pltpu.VMEM(lse.shape, F32), column, column, dma((8,)), dma((4,)), _scatter_scratch(items)],
        (x, cos, sin, dh, lse, seen, weights, [t.reshape(_cut(t.shape)) for t in terms]),
        (*_like(x), [jax.ShapeDtypeStruct(_cut(x.shape), BF)] * 4, blocks),
        (INSIDE, INSIDE, INSIDE, INSIDE, INSIDE, [OUTSIDE] * 4, [OUTSIDE] * 4, [OUTSIDE] * 3), (OUTSIDE, [OUTSIDE] * 4, [INSIDE] * len(items)))
    return dx, (*four, gate, up, down)


def _last_kernel(dx_in, q, k, v, left, right, gate, up, down, dx, *outs):
    dx[0] = dx_in[...]
    for out, ref in zip((*outs[:3], *outs[4:]), (q, k, v, gate, up, down)):
        out[0] = ref[...]
    half = left.shape[1]
    outs[3][0, :, :half] = left[...]
    outs[3][0, :, half:] = right[...]


def last(dx, blocks, shapes):
    return pl.pallas_call(_last_kernel, out_shape=[jax.ShapeDtypeStruct(s, BF) for s in shapes], in_specs=[INSIDE] * (1 + len(blocks)),
                          out_specs=[INSIDE] * len(shapes))(dx, *blocks)


def solution(mesh):
    def step(x, dy, *weights):
        shapes = [a.shape for a in (x, *weights)]
        x, dy = x[0], dy[0]
        seen, h, cos, sin, lse, whole = front(x, [w[0] for w in weights])
        dh, *terms = middle(h, dy, *whole[4:])
        dx, blocks = back(x, cos, sin, dh, lse, seen, whole[:4], terms)
        return tuple(last(dx, blocks, shapes))

    states, cut = P(("rep", "dp"), None, None), P(None, "dp", None)
    return jax.shard_map(
        step,
        mesh=mesh,
        in_specs=(states, states) + (cut,) * 7,
        out_specs=(states,) + (P("rep", "dp", None),) * 7,
        check_vma=False,
    )
```
